32 devices in a mesh: slab: 4 (over y, x), blk: 8 (over z, core).
Axes of the slice: x: 2, y: 2, z: 4, core: 2. Of those that a mesh axis runs over, the one named last changes fastest.
Arguments:
- amplitudes: bfloat16 [32, 3, 56, 128, 128], P('slab', None, 'blk'), may hold values from -6 to 6
- integrals: bfloat16 [32, 3, 1200, 1200], P(('slab', 'blk')), may hold values from -0.03125 to 0.03125
- slot_tile: int32 [56], replicated, may hold values from -1 to 99, as said below
Outputs:
- residual: float32 [3, 56, 128, 128], P(None, 'blk', 'slab')
The draws below stay inside these ranges and needn't reach their ends.
Inputs may be any that keep to these rules, and one draw needn't show every extreme that they name: `slot_tile`: each of the 55 block pairs x * 10 + y with x <= y is named by exactly one slot; every other slot holds -1.
All inputs are finite; a program needn't handle non-finite values.
Results may differ from the reference program's by a relative error of at most 0.0003.
Values may be sent and summed in bfloat16 or wider, within the bound.
A program may use at most 128 MiB of HBM per device.

```python
import jax
import jax.numpy as jnp
import numpy as np
from jax import lax

V = 1200
TILE = 128
NOUT = 3
K = 32
VB = 10
VP = 1280
NTILE = 55
SLOTS = 56


def draw_slot_tile(key, part):
    listing = [x_blk * VB + y_blk for x_blk in range(VB) for y_blk in range(x_blk, VB)]
    listing = listing + [-1] * (SLOTS - NTILE)
    table = jnp.asarray(np.array(listing, dtype=np.int32))
    placing = jax.random.permutation(key, SLOTS)
    return jnp.zeros((SLOTS,), jnp.int32).at[placing].set(table).astype(jnp.int32)


def block_scale(own_key, shape, split, least, largest):
    loudness, own = 1.0, jax.random.fold_in(own_key, 6)
    for axis_at, shards_of in split:
        heights = jnp.exp(jax.random.uniform(jax.random.fold_in(own, axis_at), (shards_of,), jnp.float32, least / len(split), largest / len(split)))
        loudness = loudness * jnp.repeat(heights, shape[axis_at] // shards_of).reshape([-1 if axis == axis_at else 1 for axis in range(len(shape))])
    return loudness


def bell_draw(rng, shape, spread, limit, cuts=(), kind=jnp.bfloat16):
    factor_of = block_scale(rng, shape, cuts, -0.22, 0.18) if cuts else 1.0
    drawn = jax.random.normal(rng, shape, jnp.float32) * spread * factor_of
    return jnp.minimum(jnp.maximum(drawn, -limit), limit).astype(kind)


def setup_inputs(seed: int = 0) -> dict:
    key_list = jax.random.split(jax.random.key(seed), 4)
    amplitudes = bell_draw(key_list[0], (K, NOUT, SLOTS, TILE, TILE), 1.0, 6.0, ((0, 4), (2, 8)))
    integrals = bell_draw(key_list[1], (K, NOUT, V, V), (K * V) ** -0.5, 0.03125, ((0, 32),))
    slot_tile = draw_slot_tile(jax.random.fold_in(key_list[3], 71), 0)
    return dict(amplitudes=amplitudes, integrals=integrals, slot_tile=slot_tile)


def strict_upper(tile_len):
    row_ids = jnp.arange(tile_len)[:, None]
    col_ids = jnp.arange(tile_len)[None, :]
    return row_ids < col_ids


def unpack(packed, slot_tile):
    tile_ids = jnp.arange(VB * VB, dtype=jnp.int32)
    matches = slot_tile[None, :] == tile_ids[:, None]
    slot_ids = jnp.arange(SLOTS, dtype=jnp.int32)[None, :]
    slot_of = jnp.sum(jnp.where(matches, slot_ids, 0), axis=1).astype(jnp.int32)
    present = jnp.any(matches, axis=1)
    tiles = jnp.where(present[:, None, None], packed[slot_of], jnp.zeros((), packed.dtype))
    on_diag = (tile_ids // VB) == (tile_ids % VB)
    keeping = jnp.logical_or(jnp.logical_not(on_diag)[:, None, None], strict_upper(TILE)[None])
    tiles = jnp.where(keeping, tiles, jnp.zeros((), packed.dtype))
    whole = tiles.reshape(VB, VB, TILE, TILE).transpose(0, 2, 1, 3).reshape(VP, VP)
    return (whole - whole.T)[:V, :V]


def reference(amplitudes, integrals, slot_tile):
    ordered = [(source, target) for source in range(NOUT) for target in range(NOUT) if source != target]

    def advance(carry, inputs):
        amp_slab, int_slab = inputs
        fulls = [unpack(amp_slab[source], slot_tile) for source in range(NOUT)]
        updated = tuple(
            carry[number] + jnp.dot(fulls[pair[0]], int_slab[pair[1]], preferred_element_type=jnp.float32)
            for number, pair in enumerate(ordered)
        )
        return updated, None

    initial = tuple(jnp.zeros((V, V), jnp.float32) for entry in ordered)
    sums = lax.scan(advance, initial, (amplitudes, integrals))[0]
    lookup = {pair: number for number, pair in enumerate(ordered)}
    safe_ids = jnp.clip(slot_tile, 0, VB * VB - 1).astype(jnp.int32)
    present = (slot_tile >= 0)[:, None, None]
    results = []
    for source in range(NOUT):
        for target in range(source + 1, NOUT):
            differ = sums[lookup[(source, target)]] - sums[lookup[(target, source)]]
            resid = differ - differ.T
            padded = jnp.pad(resid, ((0, VP - V), (0, VP - V)))
            tiles = padded.reshape(VB, TILE, VB, TILE).transpose(0, 2, 1, 3).reshape(VB * VB, TILE, TILE)
            results.append(jnp.where(present, tiles[safe_ids], jnp.zeros((), jnp.float32)))
    return jnp.stack(results).astype(jnp.float32)
```

```python
import functools

import jax
import jax.numpy as jnp
from jax import lax
from jax.experimental import pallas as pl
from jax.experimental.pallas import tpu as pltpu
from jax.sharding import PartitionSpec as P


def assemble_kernel(v_width, blocks, slot_ref, packed_ref, full_ref):
    n_slots, tile_len, _ = packed_ref.shape
    row_ids = lax.broadcasted_iota(jnp.int32, (tile_len, tile_len), 0)
    col_ids = lax.broadcasted_iota(jnp.int32, (tile_len, tile_len), 1)

    def place(slot, carry):
        tile_id = slot_ref[slot]

        @pl.when(tile_id >= 0)
        def _():
            first = lax.div(tile_id, blocks)
            second = lax.rem(tile_id, blocks)
            rows = pl.ds(pl.multiple_of(first * tile_len, tile_len), tile_len)
            cols = pl.ds(pl.multiple_of(second * tile_len, tile_len), tile_len)
            row_at = row_ids + first * tile_len
            col_at = col_ids + second * tile_len
            keep = jnp.logical_and(row_at < col_at, col_at < v_width)
            tile = jnp.where(keep, packed_ref[slot].astype(jnp.float32), 0.0)
            mirror = tile.T

            @pl.when(first == second)
            def _():
                full_ref[rows, cols] = (tile - mirror).astype(full_ref.dtype)

            @pl.when(first != second)
            def _():
                full_ref[rows, cols] = tile.astype(full_ref.dtype)
                full_ref[cols, rows] = (-mirror).astype(full_ref.dtype)

        return carry

    lax.fori_loop(0, n_slots, place, 0)


def assemble(slot_tile, packed, v_width, blocks):
    tile_len = packed.shape[-1]
    padded = blocks * tile_len
    return pl.pallas_call(
        functools.partial(assemble_kernel, v_width, blocks),
        out_shape=jax.ShapeDtypeStruct((padded, padded), packed.dtype),
        in_specs=[
            pl.BlockSpec(memory_space=pltpu.SMEM),
            pl.BlockSpec(memory_space=pltpu.VMEM),
        ],
        out_specs=pl.BlockSpec(memory_space=pltpu.VMEM),
        compiler_params=pltpu.CompilerParams(vmem_limit_bytes=24 << 20),
        cost_estimate=pl.CostEstimate(
            flops=0, bytes_accessed=4 * padded * padded, transcendentals=0
        ),
        name="assemble",
    )(slot_tile, packed)


def pair_kernel(
    blocks, n_slab, n_blk, slot_ref, left_ref, right_ref, wl_ref, wr_ref, out_ref, weights, differ
):
    padded = left_ref.shape[0]
    v_width = wl_ref.shape[-1]
    tile_len = padded // blocks
    row_part = tile_len // n_slab
    slot_dev = out_ref.shape[2]
    pad = padded - v_width
    for half, ref in enumerate((wr_ref, wl_ref)):
        base = half * padded
        vals = ref[0, 0]
        weights[pl.ds(base, v_width), pl.ds(0, v_width)] = vals if half == 0 else -vals
        if pad:
            weights[pl.ds(base, padded), pl.ds(v_width, pad)] = jnp.zeros((padded, pad), weights.dtype)
            weights[pl.ds(base + v_width, pad), :] = jnp.zeros((pad, padded), weights.dtype)

    width = 2 * tile_len if padded % (2 * tile_len) == 0 else tile_len

    def columns(step, carry):
        cols = pl.ds(pl.multiple_of(step * width, width), width)
        top = jnp.dot(left_ref[...], weights[pl.ds(0, padded), cols], preferred_element_type=jnp.float32)
        low = jnp.dot(right_ref[...], weights[pl.ds(padded, padded), cols], preferred_element_type=jnp.float32)
        differ[:, cols] = top + low
        return carry

    lax.fori_loop(0, padded // width, columns, 0)

    def pack(slot, carry):
        tile_id = slot_ref[slot]
        owner = lax.div(slot, slot_dev)
        place = lax.rem(slot, slot_dev)

        @pl.when(tile_id >= 0)
        def _():
            first = lax.div(tile_id, blocks)
            second = lax.rem(tile_id, blocks)
            rows = pl.ds(pl.multiple_of(first * tile_len, tile_len), tile_len)
            cols = pl.ds(pl.multiple_of(second * tile_len, tile_len), tile_len)
            tile = differ[rows, cols] - differ[cols, rows].T
            for slab in range(n_slab):
                part = tile[slab * row_part : (slab + 1) * row_part]
                out_ref[slab, owner, place] = part

        @pl.when(tile_id < 0)
        def _():
            for slab in range(n_slab):
                out_ref[slab, owner, place] = jnp.zeros((row_part, tile_len), jnp.float32)

        return carry

    lax.fori_loop(0, n_blk * slot_dev, pack, 0)


def pair_tiles(slot_tile, fulls, integrals, source, target, n_slab, n_blk, tile_len):
    padded = fulls[0].shape[0]
    blocks = padded // tile_len
    v_width = integrals.shape[-1]
    slot_dev = slot_tile.shape[0] // n_blk
    vmem = pl.BlockSpec(memory_space=pltpu.VMEM)

    def ints(which):
        return pl.BlockSpec((1, 1, v_width, v_width), lambda i: (0, which, 0, 0), pipeline_mode=pl.Buffered(1))

    def whole(shape):
        return pl.BlockSpec(shape, lambda i: (0,) * len(shape), pipeline_mode=pl.Buffered(1))

    out_dims = (n_slab, n_blk, slot_dev, tile_len // n_slab, tile_len)
    return pl.pallas_call(
        functools.partial(pair_kernel, blocks, n_slab, n_blk),
        grid=(1,),
        out_shape=jax.ShapeDtypeStruct(out_dims, jnp.float32),
        in_specs=[
            pl.BlockSpec(memory_space=pltpu.SMEM),
            whole((padded, padded)),
            whole((padded, padded)),
            ints(source),
            ints(target),
        ],
        out_specs=whole(out_dims),
        scratch_shapes=[
            pltpu.VMEM((2 * padded, padded), fulls[0].dtype),
            pltpu.VMEM((padded, padded), jnp.float32),
        ],
        compiler_params=pltpu.CompilerParams(vmem_limit_bytes=56 << 20),
        cost_estimate=pl.CostEstimate(
            flops=4 * padded * padded * padded, bytes_accessed=16 * padded * padded, transcendentals=0
        ),
        name="pair_tiles",
    )(slot_tile, fulls[source], fulls[target], integrals, integrals)


def local(amplitudes, integrals, slot_tile):
    n_slab = lax.axis_size("slab")
    n_blk = lax.axis_size("blk")
    n_out, slot_dev, tile_len = amplitudes.shape[1:4]
    v_width = integrals.shape[-1]
    blocks = (v_width + tile_len - 1) // tile_len
    n_slots = slot_tile.shape[0]
    fulls = []
    for source in range(n_out):
        moved = lax.all_to_all(
            amplitudes[:, source], "blk", split_axis=0, concat_axis=0, tiled=True
        )
        packed = moved.reshape(n_slots, tile_len, tile_len)
        fulls.append(assemble(slot_tile, packed, v_width, blocks))
    shares = []
    for target in range(n_out):
        for source in range(target):
            arranged = pair_tiles(
                slot_tile, fulls, integrals, source, target, n_slab, n_blk, tile_len
            )
            arranged = arranged.reshape(n_slab * n_blk, slot_dev, tile_len // n_slab, tile_len)
            share = lax.psum_scatter(arranged, ("slab", "blk"), scatter_dimension=0, tiled=True)
            shares.append((source, target, share))
    shares.sort(key=lambda item: item[:2])
    return jnp.concatenate([item[2] for item in shares])


def solution(mesh):
    return jax.shard_map(
        local,
        mesh=mesh,
        in_specs=(P("slab", None, "blk", None, None), P(("slab", "blk"), None, None, None), P()),
        out_specs=P(None, "blk", "slab", None),
        check_vma=False,
    )
```

```python
import functools

import jax
import jax.numpy as jnp
from jax import lax
from jax.experimental import pallas as pl
from jax.experimental.pallas import tpu as pltpu
from jax.sharding import PartitionSpec as P


def assemble_kernel(v_width, blocks, slot_ref, packed_ref, full_ref):
    n_blk, _, slot_dev, tile_len, _ = packed_ref.shape
    row_ids = lax.broadcasted_iota(jnp.int32, (tile_len, tile_len), 0)
    col_ids = lax.broadcasted_iota(jnp.int32, (tile_len, tile_len), 1)

    def place(slot, carry):
        tile_id = slot_ref[slot]

        @pl.when(tile_id >= 0)
        def _():
            first = lax.div(tile_id, blocks)
            second = lax.rem(tile_id, blocks)
            rows = pl.ds(pl.multiple_of(first * tile_len, tile_len), tile_len)
            cols = pl.ds(pl.multiple_of(second * tile_len, tile_len), tile_len)
            row_at = row_ids + first * tile_len
            col_at = col_ids + second * tile_len
            keep = jnp.logical_and(row_at < col_at, col_at < v_width)
            packed = packed_ref[lax.div(slot, slot_dev), 0, lax.rem(slot, slot_dev)]
            tile = jnp.where(keep, packed.astype(jnp.float32), 0.0)
            mirror = tile.T

            @pl.when(first == second)
            def _():
                full_ref[rows, cols] = (tile - mirror).astype(full_ref.dtype)

            @pl.when(first != second)
            def _():
                full_ref[rows, cols] = tile.astype(full_ref.dtype)
                full_ref[cols, rows] = (-mirror).astype(full_ref.dtype)

        return carry

    lax.fori_loop(0, n_blk * slot_dev, place, 0)


def assemble(slot_tile, packed, which, v_width, blocks):
    n_blk, _, slot_dev, tile_len, _ = packed.shape
    padded = blocks * tile_len
    return pl.pallas_call(
        functools.partial(assemble_kernel, v_width, blocks),
        grid=(1,),
        out_shape=jax.ShapeDtypeStruct((padded, padded), packed.dtype),
        in_specs=[
            pl.BlockSpec(memory_space=pltpu.SMEM),
            pl.BlockSpec(
                (n_blk, 1, slot_dev, tile_len, tile_len),
                lambda i: (0, which, 0, 0, 0),
                pipeline_mode=pl.Buffered(1),
            ),
        ],
        out_specs=pl.BlockSpec((padded, padded), lambda i: (0, 0), pipeline_mode=pl.Buffered(1)),
        compiler_params=pltpu.CompilerParams(vmem_limit_bytes=24 << 20),
        cost_estimate=pl.CostEstimate(
            flops=0, bytes_accessed=4 * padded * padded, transcendentals=0
        ),
        name="assemble",
    )(slot_tile, packed)


def pair_kernel(
    blocks, n_slab, n_blk, slot_ref, left_ref, right_ref, wl_ref, wr_ref, *rest
):
    out_ref, weights, differ = rest[-3:]
    padded = left_ref.shape[0]
    v_width = wl_ref.shape[-1]
    tile_len = padded // blocks
    row_part = tile_len // n_slab
    slot_dev = out_ref.shape[3]
    pad = padded - v_width
    for half, ref in enumerate((wr_ref, wl_ref)):
        base = half * padded
        vals = ref[0, 0]
        weights[pl.ds(base, v_width), pl.ds(0, v_width)] = vals if half == 0 else -vals
        if pad:
            weights[pl.ds(base, padded), pl.ds(v_width, pad)] = jnp.zeros((padded, pad), weights.dtype)
            weights[pl.ds(base + v_width, pad), :] = jnp.zeros((pad, padded), weights.dtype)

    width = 2 * tile_len if padded % (2 * tile_len) == 0 else tile_len

    def columns(step, carry):
        cols = pl.ds(pl.multiple_of(step * width, width), width)
        top = jnp.dot(left_ref[...], weights[pl.ds(0, padded), cols], preferred_element_type=jnp.float32)
        low = jnp.dot(right_ref[...], weights[pl.ds(padded, padded), cols], preferred_element_type=jnp.float32)
        differ[:, cols] = top + low
        return carry

    lax.fori_loop(0, padded // width, columns, 0)

    def pack(slot, carry):
        tile_id = slot_ref[slot]
        owner = lax.div(slot, slot_dev)
        place = lax.rem(slot, slot_dev)

        @pl.when(tile_id >= 0)
        def _():
            first = lax.div(tile_id, blocks)
            second = lax.rem(tile_id, blocks)
            rows = pl.ds(pl.multiple_of(first * tile_len, tile_len), tile_len)
            cols = pl.ds(pl.multiple_of(second * tile_len, tile_len), tile_len)
            tile = differ[rows, cols] - differ[cols, rows].T
            for slab in range(n_slab):
                part = tile[slab * row_part : (slab + 1) * row_part]
                out_ref[slab, owner, 0, place] = part

        @pl.when(tile_id < 0)
        def _():
            for slab in range(n_slab):
                out_ref[slab, owner, 0, place] = jnp.zeros((row_part, tile_len), jnp.float32)

        return carry

    lax.fori_loop(0, n_blk * slot_dev, pack, 0)


def pair_tiles(slot_tile, fulls, integrals, source, target, pair, n_pair, held, n_slab, n_blk, tile_len):
    padded = fulls[0].shape[0]
    blocks = padded // tile_len
    v_width = integrals.shape[-1]
    slot_dev = slot_tile.shape[0] // n_blk

    def ints(which):
        return pl.BlockSpec((1, 1, v_width, v_width), lambda i: (0, which, 0, 0), pipeline_mode=pl.Buffered(1))

    def whole(shape):
        return pl.BlockSpec(shape, lambda i: (0,) * len(shape), pipeline_mode=pl.Buffered(1))

    row_part = tile_len // n_slab
    out_dims = (n_slab, n_blk, n_pair, slot_dev, row_part, tile_len)
    more = [] if held is None else [held]
    return pl.pallas_call(
        functools.partial(pair_kernel, blocks, n_slab, n_blk),
        grid=(1,),
        out_shape=jax.ShapeDtypeStruct(out_dims, jnp.float32),
        in_specs=[
            pl.BlockSpec(memory_space=pltpu.SMEM),
            whole((padded, padded)),
            whole((padded, padded)),
            ints(source),
            ints(target),
        ]
        + [pl.BlockSpec(memory_space=pl.ANY) for _ in more],
        out_specs=pl.BlockSpec(
            (n_slab, n_blk, 1, slot_dev, row_part, tile_len),
            lambda i: (0, 0, pair, 0, 0, 0),
            pipeline_mode=pl.Buffered(1),
        ),
        input_output_aliases={5: 0} if more else {},
        scratch_shapes=[
            pltpu.VMEM((2 * padded, padded), fulls[0].dtype),
            pltpu.VMEM((padded, padded), jnp.float32),
        ],
        compiler_params=pltpu.CompilerParams(vmem_limit_bytes=56 << 20),
        cost_estimate=pl.CostEstimate(
            flops=4 * padded * padded * padded, bytes_accessed=16 * padded * padded, transcendentals=0
        ),
        name="pair_tiles",
    )(slot_tile, fulls[source], fulls[target], integrals, integrals, *more)


def local(amplitudes, integrals, slot_tile):
    n_slab = lax.axis_size("slab")
    n_blk = lax.axis_size("blk")
    n_out, slot_dev, tile_len = amplitudes.shape[1:4]
    v_width = integrals.shape[-1]
    blocks = (v_width + tile_len - 1) // tile_len
    n_slots = slot_tile.shape[0]
    row_part = tile_len // n_slab
    last = n_out - 1
    head = lax.all_to_all(amplitudes[:, :last], "blk", split_axis=0, concat_axis=0, tiled=True)
    head, rest = lax.optimization_barrier((head, amplitudes[:, last:]))
    tail = lax.all_to_all(rest, "blk", split_axis=0, concat_axis=0, tiled=True)
    fulls = [assemble(slot_tile, head, source, v_width, blocks) for source in range(last)]
    fulls.append(assemble(slot_tile, tail, 0, v_width, blocks))
    pairs = [(source, target) for source in range(n_out) for target in range(source + 1, n_out)]
    held = None
    for source, target in sorted(pairs, key=lambda pair: pair[1]):
        held = pair_tiles(
            slot_tile, fulls, integrals, source, target, pairs.index((source, target)),
            len(pairs), held, n_slab, n_blk, tile_len,
        )
    arranged = held.reshape(n_slab * n_blk, len(pairs), slot_dev, row_part, tile_len)
    share = lax.psum_scatter(arranged, ("slab", "blk"), scatter_dimension=0, tiled=True)
    return share.reshape(len(pairs), slot_dev, row_part, tile_len)


def solution(mesh):
    return jax.shard_map(
        local,
        mesh=mesh,
        in_specs=(P("slab", None, "blk", None, None), P(("slab", "blk"), None, None, None), P()),
        out_specs=P(None, "blk", "slab", None),
        check_vma=False,
    )
```
